32 devices in a mesh: lev: 4 (over y, x), col: 8 (over z, core).
Axes of the slice: x: 2, y: 2, z: 4, core: 2. Of those that a mesh axis runs over, the one named last changes fastest.
Arguments:
- control_field: float32 [96, 16, 192, 128], P('lev', None, 'col'), may hold values from -24 to 24
- decay_rate: float32 [96, 192, 128], P('lev', 'col'), may hold values from 0.5 to 0.999
- diffusivity: float32 [192, 128], P('col'), may hold values from 0.08 to 0.24
Outputs:
- localized: float32 [96, 16, 192, 128], P('lev', None, 'col')
The draws below stay inside these ranges and needn't reach their ends.
All inputs are finite; a program needn't handle non-finite values.
Results may differ from the reference program's by a relative error of at most 0.00002.
Values sent between devices are 32-bit elements; how exact they have to be, the bound alone decides.
A program may use at most 64 MiB of HBM per device.

```python
import math
import jax
import jax.numpy as jnp
from jax import lax

MEMBERS = 16
LATITUDE_ROWS = 128
SMOOTH = 4
WINDOW_LEVELS = 96
WINDOW_LONGITUDES = 192


def draw_decay_rate(key, part):
    key_scale = jax.random.fold_in(key, 11)
    key_rough = jax.random.fold_in(key, 12)
    spike_key = jax.random.fold_in(key, 13)
    depth_key = jax.random.fold_in(key, 14)
    low_scale = 4.0
    high_scale = 4.0 * WINDOW_LEVELS
    column_scale = jnp.exp(jax.random.uniform(key_scale, (1, WINDOW_LONGITUDES, LATITUDE_ROWS), jnp.float32, jnp.log(low_scale), jnp.log(high_scale)))
    roughness = jax.random.uniform(key_rough, (WINDOW_LEVELS, WINDOW_LONGITUDES, LATITUDE_ROWS), jnp.float32, 0.5, 1.5)
    decay_rates = jnp.exp(-1.0 / (column_scale * roughness))
    spike_levels = jax.random.randint(spike_key, (3,), 0, WINDOW_LEVELS)
    level_numbers = jnp.arange(WINDOW_LEVELS, dtype=jnp.int32)
    spike_present = jnp.any(level_numbers[:, None] == spike_levels[None, :], axis=1)
    spike_depth = jax.random.uniform(depth_key, (1, WINDOW_LONGITUDES, LATITUDE_ROWS), jnp.float32, 0.5, 0.8)
    decay_rates = jnp.where(spike_present[:, None, None], decay_rates * spike_depth, decay_rates)
    return jnp.clip(decay_rates, 0.5, 0.999).astype(jnp.float32)


def block_scale(rng, extent, cuts, low, high):
    gain, own = 1.0, jax.random.fold_in(rng, 6)
    for axis_at, parts in cuts:
        draws = jnp.exp(jax.random.uniform(jax.random.fold_in(own, axis_at), (parts,), jnp.float32, low / len(cuts), high / len(cuts)))
        gain = gain * jnp.repeat(draws, extent[axis_at] // parts).reshape([-1 if axis == axis_at else 1 for axis in range(len(extent))])
    return gain


def scatter_about(rng, extent, spread, most, split=(), held_as=jnp.bfloat16):
    entries = jax.random.normal(rng, extent, jnp.float32) * spread
    if len(split) > 0:
        entries = block_scale(rng, extent, split, -0.22, 0.18) * entries
    return jnp.clip(entries, min=-most, max=most).astype(held_as)


def setup_inputs(seed: int = 0) -> dict:
    seeds = jax.random.split(jax.random.key(seed), 4)
    control_field = scatter_about(seeds[0], (WINDOW_LEVELS, MEMBERS, WINDOW_LONGITUDES, LATITUDE_ROWS), 4.0, 24.0, ((0, 4), (2, 8)), jnp.float32)
    decay_rate = draw_decay_rate(jax.random.fold_in(seeds[3], 71), 0)
    diffusivity = jnp.clip(jnp.exp(math.log(0.24) - 1.0986123 * jax.random.uniform(seeds[2], (WINDOW_LONGITUDES, LATITUDE_ROWS), jnp.float32) ** block_scale(seeds[2], (WINDOW_LONGITUDES, LATITUDE_ROWS), ((0, 8),), -0.2, 0.2)), 0.08, 0.24)
    return dict(control_field=control_field, decay_rate=decay_rate, diffusivity=diffusivity)


def recursion(decay_rates, field, backward):
    def advance(state, inputs):
        weight, values = inputs
        state = weight * state + (1.0 - weight) * values
        return state, state

    start = jnp.zeros(field.shape[1:], jnp.float32)
    unused, swept = lax.scan(advance, start, (decay_rates[:, None], field), reverse=backward)
    return swept


def lat_sum(field):
    padded = jnp.pad(field, ((0, 0), (0, 0), (0, 0), (1, 1)))
    return padded[..., 2:] + padded[..., :-2]


def lon_sum(field):
    padded = jnp.pad(field, ((0, 0), (0, 0), (1, 1), (0, 0)))
    return padded[:, :, 2:] + padded[:, :, :-2]


def reference(control_field, decay_rate, diffusivity):
    filtered = control_field
    for repeat in range(2):
        filtered = recursion(decay_rate, filtered, False)
        filtered = recursion(decay_rate, filtered, True)
    current = filtered
    for position in range(SMOOTH):
        current = current + diffusivity[None, None] * (lon_sum(current) + lat_sum(current) - 4.0 * current)
    return current
```

```python
import functools
import jax
import jax.numpy as jnp
from jax import lax
from jax.experimental import pallas as pl
from jax.experimental.pallas import tpu as pltpu
from jax.sharding import PartitionSpec as P

SMOOTH = 4
MESH = pl.DeviceIdType.MESH
F32 = jnp.float32


def exchange_kernel(
    n, nc, x_hbm, w_ref, kappa_ref,
    xh_out, wh_out, kh_out, e_out, eh_out,
    xv, work, sums, coef, gathered, solved, entering,
    load_sem, coef_send, coef_recv, sum_send, sum_recv, back_send, back_recv,
    halo_send, halo_recv, edge_send, edge_recv, out_sem,
):
    levels, members, cols, lanes = xv.shape
    share = members // n
    me = lax.axis_index("lev")
    col = lax.axis_index("col")
    has_low = col > 0
    has_high = col < nc - 1
    groups = cols // 8

    load = pltpu.make_async_copy(x_hbm, xv, load_sem)
    load.start()

    barrier = pltpu.get_barrier_semaphore()
    for j in range(1, n):
        pl.semaphore_signal(barrier, inc=1, device_id={"lev": lax.rem(me + j, n)}, device_id_type=MESH)
    for step in (1, nc - 1):
        pl.semaphore_signal(barrier, inc=1, device_id={"col": lax.rem(col + step, nc)}, device_id_type=MESH)
    pl.semaphore_wait(barrier, n + 1)

    def to_high(src, dst, sem):
        return pltpu.make_async_remote_copy(
            src_ref=src, dst_ref=dst, send_sem=halo_send.at[sem], recv_sem=halo_recv.at[sem],
            device_id={"col": lax.rem(col + 1, nc)}, device_id_type=MESH)

    def to_low(src, dst, sem):
        return pltpu.make_async_remote_copy(
            src_ref=src, dst_ref=dst, send_sem=halo_send.at[sem], recv_sem=halo_recv.at[sem],
            device_id={"col": lax.rem(col + nc - 1, nc)}, device_id_type=MESH)

    s = SMOOTH
    up_copies = [
        to_high(x_hbm.at[:, :, pl.ds(cols - s, s)], xh_out.at[:, :, pl.ds(s, s)], 0),
        to_high(w_ref.at[:, pl.ds(cols - s, s)], wh_out.at[:, pl.ds(s, s)], 1),
        to_high(kappa_ref.at[pl.ds(cols - s, s)], kh_out.at[pl.ds(s, s)], 2),
    ]
    down_copies = [
        to_low(x_hbm.at[:, :, pl.ds(0, s)], xh_out.at[:, :, pl.ds(0, s)], 3),
        to_low(w_ref.at[:, pl.ds(0, s)], wh_out.at[:, pl.ds(0, s)], 4),
        to_low(kappa_ref.at[pl.ds(0, s)], kh_out.at[pl.ds(0, s)], 5),
    ]

    @pl.when(has_high)
    def _():
        for copy in up_copies:
            copy.start()

    @pl.when(has_low)
    def _():
        for copy in down_copies:
            copy.start()

    def coefficients(g, carry):
        rows = pl.ds(pl.multiple_of(g * 8, 8), 8)
        w = [w_ref[k, rows] for k in range(levels)]
        f1 = jnp.ones((8, lanes), F32)
        up = []
        for k in range(levels):
            f1 = w[k] * f1
            up.append(f1)
        alpha = f1
        a = jnp.zeros((8, lanes), F32)
        b = jnp.ones((8, lanes), F32)
        da, db = [None] * levels, [None] * levels
        for k in reversed(range(levels)):
            a = w[k] * a + (1.0 - w[k]) * up[k]
            b = w[k] * b
            da[k], db[k] = a, b
        beta = a
        a = jnp.zeros((8, lanes), F32)
        b = jnp.zeros((8, lanes), F32)
        for k in range(levels):
            a = w[k] * a + (1.0 - w[k]) * da[k]
            b = w[k] * b + (1.0 - w[k]) * db[k]
            da[k], db[k] = a, b
        delta, gamma = a, b
        a = jnp.zeros((8, lanes), F32)
        b = jnp.zeros((8, lanes), F32)
        for k in reversed(range(levels)):
            a = w[k] * a + (1.0 - w[k]) * da[k]
            b = w[k] * b + (1.0 - w[k]) * db[k]
        for i, value in enumerate((alpha, beta, gamma, delta, b, a)):
            coef[me, i, rows] = value
        return carry

    lax.fori_loop(0, groups, coefficients, 0)
    coef_copies = []
    for j in range(1, n):
        copy = pltpu.make_async_remote_copy(
            src_ref=coef.at[me], dst_ref=coef.at[me], send_sem=coef_send.at[j], recv_sem=coef_recv.at[j],
            device_id={"lev": lax.rem(me + j, n)}, device_id_type=MESH)
        copy.start()
        coef_copies.append(copy)

    load.wait()
    mb = 8

    def local(t, carry):
        g = lax.rem(t, groups)
        rows = pl.ds(pl.multiple_of(g * 8, 8), 8)
        mem = pl.ds((t // groups) * mb, mb)
        state = jnp.zeros((mb, 8, lanes), F32)
        for k in range(levels):
            w = w_ref[k, rows][None]
            state = w * state + (1.0 - w) * xv[k, mem, rows]
            work[k] = state
        sums[0, mem, rows] = state
        state = jnp.zeros((mb, 8, lanes), F32)
        for k in reversed(range(levels)):
            w = w_ref[k, rows][None]
            state = w * state + (1.0 - w) * work[k]
            work[k] = state
        sums[2, mem, rows] = state
        state = jnp.zeros((mb, 8, lanes), F32)
        for k in range(levels):
            w = w_ref[k, rows][None]
            state = w * state + (1.0 - w) * work[k]
            work[k] = state
        sums[1, mem, rows] = state
        state = jnp.zeros((mb, 8, lanes), F32)
        for k in reversed(range(levels)):
            w = w_ref[k, rows][None]
            state = w * state + (1.0 - w) * work[k]
        sums[3, mem, rows] = state
        return carry

    lax.fori_loop(0, groups * (members // mb), local, 0)

    def half(kind):
        return pl.ds(2 * kind, 2)

    def gives(kind, dev):
        return dev < n - 1 if kind == 0 else dev > 0

    def takes(kind, dev):
        return dev > 0 if kind == 0 else dev < n - 1

    def sum_copy(j, kind):
        peer = lax.rem(me + j, n)
        return pltpu.make_async_remote_copy(
            src_ref=sums.at[half(kind), pl.ds(peer * share, share)], dst_ref=gathered.at[me, half(kind)],
            send_sem=sum_send.at[j, kind], recv_sem=sum_recv.at[j, kind],
            device_id={"lev": peer}, device_id_type=MESH)

    for j in range(1, n):
        for kind in range(2):
            @pl.when(gives(kind, me))
            def _(j=j, kind=kind):
                sum_copy(j, kind).start()

    gathered[me] = sums[:, pl.ds(me * share, share)]
    for j in range(1, n):
        coef_copies[j - 1].wait_recv()
    for j in range(1, n):
        source = lax.rem(me + n - j, n)
        for kind in range(2):
            @pl.when(gives(kind, source))
            def _(j=j, kind=kind):
                sum_copy(j, kind).wait_recv()

    def solve(t, carry):
        g = lax.rem(t, groups)
        rows = pl.ds(pl.multiple_of(g * 8, 8), 8)
        m = t // groups

        def c(d, i):
            return coef[d, i, rows]

        zero = jnp.zeros((8, lanes), F32)
        f1 = [zero]
        for d in range(n - 1):
            f1.append(c(d, 0) * f1[d] + gathered[d, 0, m, rows])
        b1 = [zero] * n
        for d in range(n - 1, 0, -1):
            b1[d - 1] = c(d, 0) * b1[d] + c(d, 1) * f1[d] + gathered[d, 2, m, rows]
        f2 = [zero]
        for d in range(n - 1):
            f2.append(c(d, 0) * f2[d] + c(d, 2) * b1[d] + c(d, 3) * f1[d] + gathered[d, 1, m, rows])
        b2 = [zero] * n
        for d in range(n - 1, 0, -1):
            b2[d - 1] = (c(d, 0) * b2[d] + c(d, 1) * f2[d] + c(d, 4) * b1[d] + c(d, 5) * f1[d]
                         + gathered[d, 3, m, rows])
        for d in range(n):
            for i, value in enumerate((f1[d], f2[d], b1[d], b2[d])):
                solved[d, i, m, rows] = value
        return carry

    lax.fori_loop(0, groups * share, solve, 0)

    def back_copy(j, kind):
        peer = lax.rem(me + j, n)
        return pltpu.make_async_remote_copy(
            src_ref=solved.at[peer, half(kind)], dst_ref=entering.at[half(kind), pl.ds(me * share, share)],
            send_sem=back_send.at[j, kind], recv_sem=back_recv.at[j, kind],
            device_id={"lev": peer}, device_id_type=MESH)

    for j in range(1, n):
        peer = lax.rem(me + j, n)
        for kind in range(2):
            @pl.when(takes(kind, peer))
            def _(j=j, kind=kind):
                back_copy(j, kind).start()

    entering[:, pl.ds(me * share, share)] = solved[me]

    for kind in range(2):
        @pl.when(takes(kind, me) == False)
        def _(kind=kind):
            for j in range(1, n):
                entering[half(kind), pl.ds(lax.rem(me + j, n) * share, share)] = jnp.zeros(
                    (2, share, cols, lanes), F32)

        @pl.when(takes(kind, me))
        def _(kind=kind):
            for j in range(1, n):
                back_copy(j, kind).wait_recv()

    out = pltpu.make_async_copy(entering, e_out, out_sem)
    out.start()
    edge_high = pltpu.make_async_remote_copy(
        src_ref=entering.at[:, :, pl.ds(cols - s, s)], dst_ref=eh_out.at[:, :, pl.ds(s, s)],
        send_sem=edge_send.at[0], recv_sem=edge_recv.at[0],
        device_id={"col": lax.rem(col + 1, nc)}, device_id_type=MESH)
    edge_low = pltpu.make_async_remote_copy(
        src_ref=entering.at[:, :, pl.ds(0, s)], dst_ref=eh_out.at[:, :, pl.ds(0, s)],
        send_sem=edge_send.at[1], recv_sem=edge_recv.at[1],
        device_id={"col": lax.rem(col + nc - 1, nc)}, device_id_type=MESH)

    @pl.when(has_high)
    def _():
        edge_high.start()

    @pl.when(has_low)
    def _():
        edge_low.start()

    for j in range(1, n):
        coef_copies[j - 1].wait_send()
        for kind in range(2):
            @pl.when(gives(kind, me))
            def _(j=j, kind=kind):
                sum_copy(j, kind).wait_send()

            @pl.when(takes(kind, lax.rem(me + j, n)))
            def _(j=j, kind=kind):
                back_copy(j, kind).wait_send()

    @pl.when(has_high)
    def _():
        for copy in up_copies + [edge_high]:
            copy.wait_send()
        for copy in down_copies + [edge_low]:
            copy.wait_recv()

    @pl.when(has_low)
    def _():
        for copy in down_copies + [edge_low]:
            copy.wait_send()
        for copy in up_copies + [edge_high]:
            copy.wait_recv()

    out.wait()


def exchange(n, nc, x, w, kappa):
    levels, members, cols, lanes = x.shape
    share = members // n
    s2 = 2 * SMOOTH
    hbm = pl.BlockSpec(memory_space=pl.ANY)
    vmem = pl.BlockSpec(memory_space=pltpu.VMEM)
    dma = pltpu.SemaphoreType.DMA
    return pl.pallas_call(
        functools.partial(exchange_kernel, n, nc),
        out_shape=[
            jax.ShapeDtypeStruct((levels, members, s2, lanes), F32),
            jax.ShapeDtypeStruct((levels, s2, lanes), F32),
            jax.ShapeDtypeStruct((s2, lanes), F32),
            jax.ShapeDtypeStruct((4, members, cols, lanes), F32),
            jax.ShapeDtypeStruct((4, members, s2, lanes), F32),
        ],
        in_specs=[hbm, vmem, vmem],
        out_specs=[hbm] * 5,
        scratch_shapes=[
            pltpu.VMEM(x.shape, F32),
            pltpu.VMEM((levels, 8, 8, lanes), F32),
            pltpu.VMEM((4, members, cols, lanes), F32),
            pltpu.VMEM((n, 6, cols, lanes), F32),
            pltpu.VMEM((n, 4, share, cols, lanes), F32),
            pltpu.VMEM((n, 4, share, cols, lanes), F32),
            pltpu.VMEM((4, members, cols, lanes), F32),
            dma, dma((n,)), dma((n,)), dma((n, 2)), dma((n, 2)), dma((n, 2)), dma((n, 2)),
            dma((6,)), dma((6,)), dma((2,)), dma((2,)), dma,
        ],
        compiler_params=pltpu.CompilerParams(
            collective_id=0, has_side_effects=True, vmem_limit_bytes=40 << 20),
        name="exchange",
    )(x, w, kappa)


def finish_kernel(nc, x_ref, xh_ref, w_ref, wh_ref, k_ref, kh_ref, e_ref, eh_ref, out_ref, u_ref, wall, kall):
    levels, mb, cols, lanes = x_ref.shape
    col = lax.axis_index("col")
    wide = cols + 8
    sub = lax.broadcasted_iota(jnp.int32, (8, lanes), 0)
    first = jnp.where(col < nc - 1, 0, SMOOTH)
    last = jnp.where(col > 0, 2 * SMOOTH, SMOOTH)
    real = (sub >= first) & (sub < last)

    @pl.when(pl.program_id(0) == 0)
    def _():
        wall[:, :cols] = w_ref[...]
        wall[:, cols:] = jnp.where(real[None], wh_ref[...], 0.5)
        kall[:cols] = k_ref[...]
        kall[cols:] = jnp.where(real, kh_ref[...], 0.0)

    def columns(rows, xs, f1, f2, b1, b2):
        state = f1
        for k in range(levels):
            w = wall[k, rows][None]
            state = w * state + (1.0 - w) * xs(k)
            u_ref[k, :, rows] = state
        for state, order in ((b1, range(levels - 1, -1, -1)), (f2, range(levels)), (b2, range(levels - 1, -1, -1))):
            for k in order:
                w = wall[k, rows][None]
                state = w * state + (1.0 - w) * u_ref[k, :, rows]
                u_ref[k, :, rows] = state

    for g in range(cols // 8):
        rows = pl.ds(g * 8, 8)
        columns(rows, lambda k: x_ref[k, :, rows], *(e_ref[i, :, rows] for i in range(4)))
    keep = real[None]
    columns(pl.ds(cols, 8), lambda k: jnp.where(keep, xh_ref[k], 0.0),
            *(jnp.where(keep, eh_ref[i], 0.0) for i in range(4)))

    lane = lax.broadcasted_iota(jnp.int32, (wide, lanes), 1)
    kappa = kall[...]
    middle = (1.0 - 4.0 * kappa)[None]
    south = jnp.where(lane > 0, kappa, 0.0)[None]
    north = jnp.where(lane < lanes - 1, kappa, 0.0)[None]
    kappa = kappa[None]

    def diffuse(k, carry):
        u = u_ref[k]
        for step in range(SMOOTH):
            u = (middle * u + kappa * (pltpu.roll(u, 1, 1) + pltpu.roll(u, wide - 1, 1))
                 + south * pltpu.roll(u, 1, 2) + north * pltpu.roll(u, lanes - 1, 2))
        out_ref[k] = u[:, :cols]
        return carry

    lax.fori_loop(0, levels, diffuse, 0)


def finish(nc, x, xh, w, wh, kappa, kh, e, eh):
    levels, members, cols, lanes = x.shape
    mb = 2

    def by_member(shape):
        return pl.BlockSpec((shape[0], mb) + shape[2:], lambda i: (0, i, 0, 0))

    def whole(shape):
        return pl.BlockSpec(shape, lambda i: (0,) * len(shape))

    return pl.pallas_call(
        functools.partial(finish_kernel, nc),
        grid=(members // mb,),
        out_shape=jax.ShapeDtypeStruct(x.shape, F32),
        in_specs=[by_member(x.shape), by_member(xh.shape), whole(w.shape), whole(wh.shape),
                  whole(kappa.shape), whole(kh.shape), by_member(e.shape), by_member(eh.shape)],
        out_specs=by_member(x.shape),
        scratch_shapes=[
            pltpu.VMEM((levels, mb, cols + 8, lanes), F32),
            pltpu.VMEM((levels, cols + 8, lanes), F32),
            pltpu.VMEM((cols + 8, lanes), F32),
        ],
        compiler_params=pltpu.CompilerParams(vmem_limit_bytes=40 << 20),
        name="finish",
    )(x, xh, w, wh, kappa, kh, e, eh)


def solution(mesh):
    n, nc = mesh.shape["lev"], mesh.shape["col"]

    def per_device(x, w, kappa):
        xh, wh, kh, e, eh = exchange(n, nc, x, w, kappa)
        return finish(nc, x, xh, w, wh, kappa, kh, e, eh)

    in_specs = (P("lev", None, "col", None), P("lev", "col", None), P("col", None))
    out_specs = P("lev", None, "col", None)
    return jax.shard_map(per_device, mesh=mesh, in_specs=in_specs, out_specs=out_specs, check_vma=False)
```

```python
import functools
import jax
import jax.numpy as jnp
from jax import lax
from jax.experimental import pallas as pl
from jax.experimental.pallas import tpu as pltpu
from jax.sharding import PartitionSpec as P

SMOOTH = 4
MESH = pl.DeviceIdType.MESH
F32 = jnp.float32


def exchange_kernel(
    n, nc, x_hbm, w_ref, kappa_ref,
    xh_out, wh_out, kh_out, e_out, eh_out,
    xv, work, sums, coef, gathered, solved, entering,
    load_sem, coef_send, coef_recv, sum_send, sum_recv, back_send, back_recv,
    halo_send, halo_recv, edge_send, edge_recv, out_sem,
):
    levels, members, cols, lanes = xv.shape
    share = members // n
    me = lax.axis_index("lev")
    col = lax.axis_index("col")
    has_low = col > 0
    has_high = col < nc - 1
    groups = cols // 8

    load = pltpu.make_async_copy(x_hbm, xv, load_sem)
    load.start()

    barrier = pltpu.get_barrier_semaphore()
    for j in range(1, n):
        pl.semaphore_signal(barrier, inc=1, device_id={"lev": lax.rem(me + j, n)}, device_id_type=MESH)
    for step in (1, nc - 1):
        pl.semaphore_signal(barrier, inc=1, device_id={"col": lax.rem(col + step, nc)}, device_id_type=MESH)
    pl.semaphore_wait(barrier, n + 1)

    def to_high(src, dst, sem):
        return pltpu.make_async_remote_copy(
            src_ref=src, dst_ref=dst, send_sem=halo_send.at[sem], recv_sem=halo_recv.at[sem],
            device_id={"col": lax.rem(col + 1, nc)}, device_id_type=MESH)

    def to_low(src, dst, sem):
        return pltpu.make_async_remote_copy(
            src_ref=src, dst_ref=dst, send_sem=halo_send.at[sem], recv_sem=halo_recv.at[sem],
            device_id={"col": lax.rem(col + nc - 1, nc)}, device_id_type=MESH)

    s = SMOOTH
    up_copies = [
        to_high(x_hbm.at[:, :, pl.ds(cols - s, s)], xh_out.at[:, :, pl.ds(s, s)], 0),
        to_high(w_ref.at[:, pl.ds(cols - s, s)], wh_out.at[:, pl.ds(s, s)], 1),
        to_high(kappa_ref.at[pl.ds(cols - s, s)], kh_out.at[pl.ds(s, s)], 2),
    ]
    down_copies = [
        to_low(x_hbm.at[:, :, pl.ds(0, s)], xh_out.at[:, :, pl.ds(0, s)], 3),
        to_low(w_ref.at[:, pl.ds(0, s)], wh_out.at[:, pl.ds(0, s)], 4),
        to_low(kappa_ref.at[pl.ds(0, s)], kh_out.at[pl.ds(0, s)], 5),
    ]

    @pl.when(has_high)
    def _():
        for copy in up_copies:
            copy.start()

    @pl.when(has_low)
    def _():
        for copy in down_copies:
            copy.start()

    def coefficients(g, carry):
        rows = pl.ds(pl.multiple_of(g * 8, 8), 8)
        w = [w_ref[k, rows] for k in range(levels)]
        f1 = jnp.ones((8, lanes), F32)
        up = []
        for k in range(levels):
            f1 = w[k] * f1
            up.append(f1)
        alpha = f1
        a = jnp.zeros((8, lanes), F32)
        b = jnp.ones((8, lanes), F32)
        da, db = [None] * levels, [None] * levels
        for k in reversed(range(levels)):
            a = w[k] * a + (1.0 - w[k]) * up[k]
            b = w[k] * b
            da[k], db[k] = a, b
        beta = a
        a = jnp.zeros((8, lanes), F32)
        b = jnp.zeros((8, lanes), F32)
        for k in range(levels):
            a = w[k] * a + (1.0 - w[k]) * da[k]
            b = w[k] * b + (1.0 - w[k]) * db[k]
            da[k], db[k] = a, b
        delta, gamma = a, b
        a = jnp.zeros((8, lanes), F32)
        b = jnp.zeros((8, lanes), F32)
        for k in reversed(range(levels)):
            a = w[k] * a + (1.0 - w[k]) * da[k]
            b = w[k] * b + (1.0 - w[k]) * db[k]
        for i, value in enumerate((alpha, beta, gamma, delta, b, a)):
            coef[me, i, rows] = value
        return carry

    lax.fori_loop(0, groups, coefficients, 0)
    coef_copies = []
    for j in range(1, n):
        copy = pltpu.make_async_remote_copy(
            src_ref=coef.at[me], dst_ref=coef.at[me], send_sem=coef_send.at[j], recv_sem=coef_recv.at[j],
            device_id={"lev": lax.rem(me + j, n)}, device_id_type=MESH)
        copy.start()
        coef_copies.append(copy)

    load.wait()
    mb = 8

    def local(t, carry):
        g = lax.rem(t, groups)
        rows = pl.ds(pl.multiple_of(g * 8, 8), 8)
        mem = pl.ds((t // groups) * mb, mb)
        state = jnp.zeros((mb, 8, lanes), F32)
        for k in range(levels):
            w = w_ref[k, rows][None]
            state = w * state + (1.0 - w) * xv[k, mem, rows]
            work[k] = state
        sums[0, mem, rows] = state
        state = jnp.zeros((mb, 8, lanes), F32)
        for k in reversed(range(levels)):
            w = w_ref[k, rows][None]
            state = w * state + (1.0 - w) * work[k]
            work[k] = state
        sums[2, mem, rows] = state
        state = jnp.zeros((mb, 8, lanes), F32)
        for k in range(levels):
            w = w_ref[k, rows][None]
            state = w * state + (1.0 - w) * work[k]
            work[k] = state
        sums[1, mem, rows] = state
        state = jnp.zeros((mb, 8, lanes), F32)
        for k in reversed(range(levels)):
            w = w_ref[k, rows][None]
            state = w * state + (1.0 - w) * work[k]
        sums[3, mem, rows] = state
        return carry

    lax.fori_loop(0, groups * (members // mb), local, 0)

    def half(kind):
        return pl.ds(2 * kind, 2)

    def gives(kind, dev):
        return dev < n - 1 if kind == 0 else dev > 0

    def takes(kind, dev):
        return dev > 0 if kind == 0 else dev < n - 1

    def sum_copy(j, kind):
        peer = lax.rem(me + j, n)
        return pltpu.make_async_remote_copy(
            src_ref=sums.at[half(kind), pl.ds(peer * share, share)], dst_ref=gathered.at[me, half(kind)],
            send_sem=sum_send.at[j, kind], recv_sem=sum_recv.at[j, kind],
            device_id={"lev": peer}, device_id_type=MESH)

    for j in range(1, n):
        for kind in range(2):
            @pl.when(gives(kind, me))
            def _(j=j, kind=kind):
                sum_copy(j, kind).start()

    gathered[me] = sums[:, pl.ds(me * share, share)]
    for j in range(1, n):
        coef_copies[j - 1].wait_recv()
    for j in range(1, n):
        source = lax.rem(me + n - j, n)
        for kind in range(2):
            @pl.when(gives(kind, source))
            def _(j=j, kind=kind):
                sum_copy(j, kind).wait_recv()

    def solve(t, carry):
        g = lax.rem(t, groups)
        rows = pl.ds(pl.multiple_of(g * 8, 8), 8)
        m = t // groups

        def c(d, i):
            return coef[d, i, rows]

        zero = jnp.zeros((8, lanes), F32)
        f1 = [zero]
        for d in range(n - 1):
            f1.append(c(d, 0) * f1[d] + gathered[d, 0, m, rows])
        b1 = [zero] * n
        for d in range(n - 1, 0, -1):
            b1[d - 1] = c(d, 0) * b1[d] + c(d, 1) * f1[d] + gathered[d, 2, m, rows]
        f2 = [zero]
        for d in range(n - 1):
            f2.append(c(d, 0) * f2[d] + c(d, 2) * b1[d] + c(d, 3) * f1[d] + gathered[d, 1, m, rows])
        b2 = [zero] * n
        for d in range(n - 1, 0, -1):
            b2[d - 1] = (c(d, 0) * b2[d] + c(d, 1) * f2[d] + c(d, 4) * b1[d] + c(d, 5) * f1[d]
                         + gathered[d, 3, m, rows])
        for d in range(n):
            for i, value in enumerate((f1[d], f2[d], b1[d], b2[d])):
                solved[d, i, m, rows] = value
        return carry

    lax.fori_loop(0, groups * share, solve, 0)

    def back_copy(j, kind):
        peer = lax.rem(me + j, n)
        return pltpu.make_async_remote_copy(
            src_ref=solved.at[peer, half(kind)], dst_ref=entering.at[half(kind), pl.ds(me * share, share)],
            send_sem=back_send.at[j, kind], recv_sem=back_recv.at[j, kind],
            device_id={"lev": peer}, device_id_type=MESH)

    for j in range(1, n):
        peer = lax.rem(me + j, n)
        for kind in range(2):
            @pl.when(takes(kind, peer))
            def _(j=j, kind=kind):
                back_copy(j, kind).start()

    entering[:, pl.ds(me * share, share)] = solved[me]

    for kind in range(2):
        @pl.when(takes(kind, me) == False)
        def _(kind=kind):
            for j in range(1, n):
                entering[half(kind), pl.ds(lax.rem(me + j, n) * share, share)] = jnp.zeros(
                    (2, share, cols, lanes), F32)

        @pl.when(takes(kind, me))
        def _(kind=kind):
            for j in range(1, n):
                back_copy(j, kind).wait_recv()

    out = pltpu.make_async_copy(entering, e_out, out_sem)
    out.start()
    edge_high = pltpu.make_async_remote_copy(
        src_ref=entering.at[:, :, pl.ds(cols - s, s)], dst_ref=eh_out.at[:, :, pl.ds(s, s)],
        send_sem=edge_send.at[0], recv_sem=edge_recv.at[0],
        device_id={"col": lax.rem(col + 1, nc)}, device_id_type=MESH)
    edge_low = pltpu.make_async_remote_copy(
        src_ref=entering.at[:, :, pl.ds(0, s)], dst_ref=eh_out.at[:, :, pl.ds(0, s)],
        send_sem=edge_send.at[1], recv_sem=edge_recv.at[1],
        device_id={"col": lax.rem(col + nc - 1, nc)}, device_id_type=MESH)

    @pl.when(has_high)
    def _():
        edge_high.start()

    @pl.when(has_low)
    def _():
        edge_low.start()

    for j in range(1, n):
        coef_copies[j - 1].wait_send()
        for kind in range(2):
            @pl.when(gives(kind, me))
            def _(j=j, kind=kind):
                sum_copy(j, kind).wait_send()

            @pl.when(takes(kind, lax.rem(me + j, n)))
            def _(j=j, kind=kind):
                back_copy(j, kind).wait_send()

    @pl.when(has_high)
    def _():
        for copy in up_copies + [edge_high]:
            copy.wait_send()
        for copy in down_copies + [edge_low]:
            copy.wait_recv()

    @pl.when(has_low)
    def _():
        for copy in down_copies + [edge_low]:
            copy.wait_send()
        for copy in up_copies + [edge_high]:
            copy.wait_recv()

    out.wait()


def exchange(n, nc, x, w, kappa):
    levels, members, cols, lanes = x.shape
    share = members // n
    s2 = 2 * SMOOTH
    hbm = pl.BlockSpec(memory_space=pl.ANY)
    vmem = pl.BlockSpec(memory_space=pltpu.VMEM)
    dma = pltpu.SemaphoreType.DMA
    return pl.pallas_call(
        functools.partial(exchange_kernel, n, nc),
        out_shape=[
            jax.ShapeDtypeStruct((levels, members, s2, lanes), F32),
            jax.ShapeDtypeStruct((levels, s2, lanes), F32),
            jax.ShapeDtypeStruct((s2, lanes), F32),
            jax.ShapeDtypeStruct((4, members, cols, lanes), F32),
            jax.ShapeDtypeStruct((4, members, s2, lanes), F32),
        ],
        in_specs=[pl.BlockSpec(memory_space=pltpu.HBM), vmem, vmem],
        out_specs=[hbm] * 5,
        scratch_shapes=[
            pltpu.VMEM(x.shape, F32),
            pltpu.VMEM((levels, 8, 8, lanes), F32),
            pltpu.VMEM((4, members, cols, lanes), F32),
            pltpu.VMEM((n, 6, cols, lanes), F32),
            pltpu.VMEM((n, 4, share, cols, lanes), F32),
            pltpu.VMEM((n, 4, share, cols, lanes), F32),
            pltpu.VMEM((4, members, cols, lanes), F32),
            dma, dma((n,)), dma((n,)), dma((n, 2)), dma((n, 2)), dma((n, 2)), dma((n, 2)),
            dma((6,)), dma((6,)), dma((2,)), dma((2,)), dma,
        ],
        compiler_params=pltpu.CompilerParams(
            collective_id=0, has_side_effects=True, vmem_limit_bytes=40 << 20),
        name="exchange",
    )(x, w, kappa)


def finish_kernel(nc, x_ref, xh_ref, w_ref, wh_ref, k_ref, kh_ref, e_ref, eh_ref, out_ref, a_ref, b_ref, wall, kall):
    levels, mb, cols, lanes = x_ref.shape
    col = lax.axis_index("col")
    sub = lax.broadcasted_iota(jnp.int32, (8, lanes), 0)
    first = jnp.where(col < nc - 1, 0, SMOOTH)
    last = jnp.where(col > 0, 2 * SMOOTH, SMOOTH)
    real = (sub >= first) & (sub < last)
    low, main, high = 8, 16, 16 + cols

    @pl.when(pl.program_id(0) == 0)
    def _():
        wall[:, :cols] = w_ref[...]
        wall[:, cols:] = jnp.where(real[None], wh_ref[...], 0.5)
        lane = lax.broadcasted_iota(jnp.int32, (cols + 8, lanes), 1)
        kappa = jnp.concatenate([k_ref[...], jnp.where(real, kh_ref[...], 0.0)], axis=0)
        kall[0] = kappa
        kall[1] = 1.0 - 4.0 * kappa
        kall[2] = jnp.where(lane > 0, kappa, 0.0)
        kall[3] = jnp.where(lane < lanes - 1, kappa, 0.0)

    keep = real[None]

    def start(i):
        return jnp.concatenate([e_ref[i], jnp.where(keep, eh_ref[i], 0.0)], axis=1)

    span = pl.ds(main, cols + 8)
    state = start(0)
    for k in range(levels):
        w = wall[k][None]
        x = jnp.concatenate([x_ref[k], jnp.where(keep, xh_ref[k], 0.0)], axis=1)
        state = w * state + (1.0 - w) * x
        a_ref[k, :, span] = state
    for i in (2, 1, 3):
        state = start(i)
        for k in range(levels) if i == 1 else reversed(range(levels)):
            w = wall[k][None]
            state = w * state + (1.0 - w) * a_ref[k, :, span]
            a_ref[k, :, span] = state
            if i == 3:
                a_ref[k, :, pl.ds(low, 8)] = state[:, cols:]

    upper = sub < SMOOTH

    chunk = max(c for c in range(1, 9) if levels % c == 0)

    def tile(src, k, m, at, rows, east, west):
        u = src[k, m, pl.ds(at, 8)]
        return (kall[1, rows] * u + kall[0, rows] * (east + west)
                + kall[2, rows] * pltpu.roll(u, 1, 1) + kall[3, rows] * pltpu.roll(u, lanes - 1, 1))

    for step in range(SMOOTH):
        src, dst = (a_ref, b_ref) if step % 2 == 0 else (b_ref, a_ref)
        final = step == SMOOTH - 1

        def body(c, carry, src=src, dst=dst, final=final):
            for dk in range(chunk):
                k = c * chunk + dk
                for m in range(mb):
                    for g in range(cols // 8):
                        at = main + 8 * g
                        rows = pl.ds(8 * g, 8)
                        value = tile(src, k, m, at, rows, src[k, m, pl.ds(at + 1, 8)], src[k, m, pl.ds(at - 1, 8)])
                        if final:
                            out_ref[k, m, rows] = value
                        else:
                            dst[k, m, pl.ds(at, 8)] = value
                    if not final:
                        east = jnp.where(upper, src[k, m, pl.ds(high + 1, 8)], src[k, m, pl.ds(low + 1, 8)])
                        west = jnp.where(upper, src[k, m, pl.ds(high - 1, 8)], src[k, m, pl.ds(low - 1, 8)])
                        value = tile(src, k, m, high, pl.ds(cols, 8), east, west)
                        dst[k, m, pl.ds(high, 8)] = value
                        dst[k, m, pl.ds(low, 8)] = value
            return carry

        lax.fori_loop(0, levels // chunk, body, 0)


def finish(nc, x, xh, w, wh, kappa, kh, e, eh):
    levels, members, cols, lanes = x.shape
    mb = 4

    def by_member(shape):
        return pl.BlockSpec((shape[0], mb) + shape[2:], lambda i: (0, i, 0, 0))

    def whole(shape):
        return pl.BlockSpec(shape, lambda i: (0,) * len(shape))

    return pl.pallas_call(
        functools.partial(finish_kernel, nc),
        grid=(members // mb,),
        out_shape=jax.ShapeDtypeStruct(x.shape, F32),
        in_specs=[by_member(x.shape), by_member(xh.shape), whole(w.shape), whole(wh.shape),
                  whole(kappa.shape), whole(kh.shape), by_member(e.shape), by_member(eh.shape)],
        out_specs=by_member(x.shape),
        scratch_shapes=[
            pltpu.VMEM((levels, mb, cols + 32, lanes), F32),
            pltpu.VMEM((levels, mb, cols + 32, lanes), F32),
            pltpu.VMEM((levels, cols + 8, lanes), F32),
            pltpu.VMEM((4, cols + 8, lanes), F32),
        ],
        compiler_params=pltpu.CompilerParams(vmem_limit_bytes=40 << 20),
        name="finish",
    )(x, xh, w, wh, kappa, kh, e, eh)


def solution(mesh):
    n, nc = mesh.shape["lev"], mesh.shape["col"]

    def per_device(x, w, kappa):
        xh, wh, kh, e, eh = exchange(n, nc, x, w, kappa)
        return finish(nc, x, xh, w, wh, kappa, kh, e, eh)

    in_specs = (P("lev", None, "col", None), P("lev", "col", None), P("col", None))
    out_specs = P("lev", None, "col", None)
    return jax.shard_map(per_device, mesh=mesh, in_specs=in_specs, out_specs=out_specs, check_vma=False)
```
